256 devices in a mesh: row: 8 (over y_hi, x), col: 32 (over z, y_lo, core).
Axes of the slice: x: 4, y: 4 (y_hi: 2, y_lo: 2; y = y_hi * 2 + y_lo), z: 8, core: 2. Of those that a mesh axis runs over, the one named last changes fastest.
Arguments:
- gradient: bfloat16 [2304, 18432], P('row', 'col'), may hold values from -6 to 6
- left_basis: bfloat16 [2304, 2304], P('row'), may hold values from -0.125 to 0.125
- right_basis: bfloat16 [18432, 18432], P('col', 'row'), may hold values from -0.046875 to 0.046875
- first_moment: float32 [2304, 18432], P('col', 'row'), may hold values from -3 to 3
- second_moment: float32 [2304, 18432], P('col', 'row'), may hold values from 0.25 to 4
Outputs:
- update: bfloat16 [2304, 18432], P('row', 'col')
- first_new: float32 [2304, 18432], P('col', 'row')
- second_new: float32 [2304, 18432], P('col', 'row')
The draws below stay inside these ranges and needn't reach their ends.
All inputs are finite; a program needn't handle non-finite values.
Results may differ from the reference program's by a relative error of at most 0.018.
Values may be sent and summed in bfloat16 or wider, within the bound.
No kernel may reach another device: no remote copies, remote signals or barrier semaphores. Data moves between devices by JAX's collectives and lax.ppermute only.
A program may use at most 64 MiB of HBM per device.

```python
import math
import jax
import jax.numpy as jnp
from jax import lax

M = 2304
N = 18432
N_ROW = 8
N_COL = 32


def levels(key, dims, cuts, low, top_value):
    gain = 1.0
    for axis_at, parts in cuts:
        draws = jax.random.uniform(jax.random.fold_in(jax.random.fold_in(key, 6), axis_at), (parts,), jnp.float32, low / len(cuts), top_value / len(cuts))
        gain = gain * jnp.repeat(jnp.exp(draws), dims[axis_at] // parts).reshape((-1,) + (1,) * (len(dims) - 1 - axis_at))
    return gain


def normal_values(own_key, extent, spread, reach, pieces=(), kind=jnp.bfloat16):
    result = jax.random.normal(own_key, extent, jnp.float32) * spread
    if len(pieces) > 0:
        result = levels(own_key, extent, pieces, -0.22, 0.18) * result
    return jnp.clip(result, min=-reach, max=reach).astype(kind)


def setup_inputs(seed: int = 0) -> dict:
    arg_keys = jax.random.split(jax.random.key(seed), 6)
    gradient = normal_values(arg_keys[0], (M, N), 1.0, 6.0, ((0, 8), (1, 32)))
    left_basis = normal_values(arg_keys[1], (M, M), M ** -0.5, 0.125, ((0, 8),))
    right_basis = normal_values(arg_keys[2], (N, N), N ** -0.5, 0.046875, ((0, 32), (1, 8)))
    first_moment = normal_values(arg_keys[3], (M, N), 0.5, 3.0, ((0, 32), (1, 8)), jnp.float32)
    second_moment = jnp.clip(jnp.exp(math.log(4.0) - 2.7725887 * jax.random.uniform(arg_keys[4], (M, N), jnp.float32) ** levels(arg_keys[4], (M, N), ((0, 32), (1, 8)), -0.2, 0.2)), 0.25, 4.0)
    return {"gradient": gradient, "left_basis": left_basis, "right_basis": right_basis, "first_moment": first_moment, "second_moment": second_moment}


beta_one = 0.9
beta_two = 0.95
epsilon = 1e-08
correct_one = 1.0 - 0.9 ** 10
correct_two = 1.0 - 0.95 ** 10

def rounded(values):
    narrow = lax.optimization_barrier(values.astype(jnp.bfloat16))
    return narrow.astype(jnp.float32)

def reference(gradient, left_basis, right_basis, first_moment, second_moment):
    precise = lax.Precision.HIGHEST
    grad_wide = gradient.astype(jnp.float32)
    left_wide = left_basis.astype(jnp.float32)
    right_wide = right_basis.astype(jnp.float32)
    row_block = M // N_ROW
    col_block = N // N_COL

    def left_part(running, block_index):
        offset = (block_index * row_block).astype(jnp.int32)
        basis_rows = lax.dynamic_slice_in_dim(left_wide, offset, row_block, 0)
        grad_rows = lax.dynamic_slice_in_dim(grad_wide, offset, row_block, 0)
        partial_value = lax.dot_general(basis_rows, grad_rows, (((0,), (0,)), ((), ())), precision=precise)
        return (running + rounded(partial_value), None)
    summed, _ = lax.scan(left_part, jnp.zeros((M, N), jnp.float32), jnp.arange(N_ROW, dtype=jnp.int32))
    rotated_left = rounded(summed)

    def right_part(running, block_index):
        offset = (block_index * col_block).astype(jnp.int32)
        left_cols = lax.dynamic_slice_in_dim(rotated_left, offset, col_block, 1)
        basis_rows = lax.dynamic_slice_in_dim(right_wide, offset, col_block, 0)
        partial_value = jnp.dot(left_cols, basis_rows, precision=precise)
        return (running + rounded(partial_value), None)
    summed, _ = lax.scan(right_part, jnp.zeros((M, N), jnp.float32), jnp.arange(N_COL, dtype=jnp.int32))
    rotated = rounded(summed)
    first_new = beta_one * first_moment + (1.0 - beta_one) * rotated
    second_new = beta_two * second_moment + (1.0 - beta_two) * rotated * rotated
    step_rot = rounded(first_new / correct_one / (jnp.sqrt(second_new / correct_two) + epsilon))

    def back_part(running, block_index):
        offset = (block_index * (N // N_ROW)).astype(jnp.int32)
        step_cols = lax.dynamic_slice_in_dim(step_rot, offset, N // N_ROW, 1)
        basis_cols = lax.dynamic_slice_in_dim(right_wide, offset, N // N_ROW, 1)
        partial_value = lax.dot_general(step_cols, basis_cols, (((1,), (1,)), ((), ())), precision=precise)
        return (running + rounded(partial_value), None)
    summed, _ = lax.scan(back_part, jnp.zeros((M, N), jnp.float32), jnp.arange(N_ROW, dtype=jnp.int32))
    back_rot = rounded(summed)
    update = jnp.dot(left_wide, back_rot, precision=precise).astype(jnp.bfloat16)
    return (update, first_new, second_new)
```

```python
import jax
import jax.numpy as jnp
from jax import lax
from jax.sharding import Mesh, PartitionSpec as P


CHUNKS = 1
beta_one = 0.9
beta_two = 0.95
epsilon = 1e-08
correct_one = 1.0 - 0.9**10
correct_two = 1.0 - 0.95**10
wide = jnp.float32
half = jnp.bfloat16


def shift(value, axis, by):
    size = lax.axis_size(axis)
    return lax.ppermute(value, axis, [(i, (i + by) % size) for i in range(size)])


def pick(blocks, index, dim=0):
    return lax.dynamic_index_in_dim(blocks, index, dim, keepdims=False)


def add(*terms):
    total = terms[0].astype(wide)
    for term in terms[1:]:
        total = total + term.astype(wide)
    return total.astype(half)


def row_sum(block_of):
    x = lax.axis_index("x")
    yh = lax.axis_index("yh")
    own, right, far, left = (block_of((x + k) % 4) for k in range(4))
    up = shift(far[0], "x", 1)
    down = shift(far[1], "x", -1)
    from_left = shift(jnp.stack([add(right[0], up), right[1]]), "x", 1)
    from_right = shift(jnp.stack([left[0], add(left[1], down)]), "x", -1)
    total = own.astype(wide) + from_left.astype(wide) + from_right.astype(wide)
    sent = pick(total, 1 - yh).astype(half)
    return (pick(total, yh) + shift(sent, "yh", 1).astype(wide)).astype(half)


def row_gather(piece):
    yh = lax.axis_index("yh")
    other = shift(piece, "yh", 1)
    first = yh == 0
    pair = jnp.stack([jnp.where(first, piece, other), jnp.where(first, other, piece)])
    left = shift(pair, "x", 1)
    right = shift(pair, "x", -1)
    far = jnp.stack([shift(left[0], "x", 1), shift(right[1], "x", -1)])
    return jnp.stack([pair, right, far, left], axis=1)


def column_sum(block_of):
    z = lax.axis_index("z")
    block = lambda k: block_of((z + k) % 8)
    far = block(4)
    n = far.shape[1] // 2
    up = shift(far[:, :n], "z", 1)
    down = shift(far[:, n:], "z", -1)
    b = block(3)
    up = shift(jnp.concatenate([add(b[:, :n], up), b[:, n:]], axis=1), "z", 1)
    b = block(-3)
    down = shift(jnp.concatenate([b[:, :n], add(b[:, n:], down)], axis=1), "z", -1)
    for k in (2, 1):
        up = shift(add(block(k), up), "z", 1)
        down = shift(add(block(-k), down), "z", -1)
    return add(block(0), up, down)


def column_gather(piece):
    n = piece.shape[1] // 2
    got = {0: piece}
    up = down = piece
    for k in (1, 2, 3):
        up = got[8 - k] = shift(up, "z", 1)
        down = got[k] = shift(down, "z", -1)
    got[4] = jnp.concatenate([shift(up[:, :n], "z", 1), shift(down[:, n:], "z", -1)], axis=1)
    return jnp.stack([got[k] for k in range(8)])


def to_quarter(blocks):
    yl, core = lax.axis_index("yl"), lax.axis_index("core")
    kept = pick(blocks, core, 1)
    other = shift(pick(blocks, 1 - core, 1), "core", 1)
    both = jnp.concatenate([kept, other], axis=2)
    return jnp.concatenate([pick(both, yl), shift(pick(both, 1 - yl), "yl", 1)], axis=1)


def from_quarter(rows):
    yl, core = lax.axis_index("yl"), lax.axis_index("core")
    n = rows.shape[1] // 4
    own, other = rows[:, : 2 * n], shift(rows[:, 2 * n :], "yl", 1)
    first = yl == 0
    pair = jnp.stack([jnp.where(first, own, other), jnp.where(first, other, own)])
    own, other = pair[:, :, :n], shift(pair[:, :, n:], "core", 1)
    first = core == 0
    return jnp.stack([jnp.where(first, own, other), jnp.where(first, other, own)], axis=1)


def step_of(rotated, first_moment, second_moment):
    rotated = rotated.astype(wide)
    first_new = beta_one * first_moment + (1.0 - beta_one) * rotated
    second_new = beta_two * second_moment + (1.0 - beta_two) * rotated * rotated
    step = first_new / correct_one / (jnp.sqrt(second_new / correct_two) + epsilon)
    return step.astype(half), first_new, second_new


def per_device(gradient, left_basis, right_basis, first_moment, second_moment):
    x, yh, z = (lax.axis_index(a) for a in ("x", "yh", "z"))
    n_cols = gradient.shape[1]
    rows = first_moment.shape[0]
    h = rows // CHUNKS
    core_basis = shift(right_basis, "core", 1)
    cut = right_basis.shape[0] // 2
    yl_basis = jnp.concatenate([shift(right_basis[:cut], "yl", 1), shift(right_basis[cut:], "yl", 1)])
    basis = jnp.concatenate([right_basis, core_basis, yl_basis, shift(yl_basis, "core", 1)])

    left_part = lax.dot_general(left_basis, gradient, (((0,), (0,)), ((), ())), preferred_element_type=wide)
    left_part = left_part.astype(half).reshape(2, 4, 2, 2, CHUNKS, h, n_cols)
    firsts, seconds, backs = [], [], []
    for j in range(CHUNKS):
        own_left = row_sum(lambda at: pick(left_part[:, :, :, :, j], at, 1))
        left = row_gather(to_quarter(own_left))
        right_part = jnp.dot(left.reshape(8 * h, -1), basis, preferred_element_type=wide).astype(half)
        right_part = right_part.reshape(2, 4, h, -1)
        rotated = column_sum(lambda at: pick(pick(right_part, at // 4, 0), (at - x) % 4, 0))
        span = slice(j * h, (j + 1) * h)
        step, first_new, second_new = step_of(rotated, first_moment[span], second_moment[span])
        firsts.append(first_new)
        seconds.append(second_new)
        steps = column_gather(step)
        back_part = lax.dot_general(
            steps.reshape(8 * h, -1), basis, (((1,), (1,)), ((), ())), preferred_element_type=wide
        ).astype(half)
        back_part = back_part.reshape(8, h, -1)
        back_own = row_sum(
            lambda at: jnp.stack([pick(back_part, (at - z) % 8), pick(back_part, (at + 4 - z) % 8)])
        )
        back = row_gather(from_quarter(back_own))
        backs.append(jnp.stack([pick(back, (k - x) % 4, 1) for k in range(4)], axis=1))
    back = jnp.stack(backs, axis=4).reshape(-1, n_cols)
    update = jnp.dot(left_basis, back, preferred_element_type=wide).astype(half)
    return update, jnp.concatenate(firsts), jnp.concatenate(seconds)


def solution(mesh):
    own = Mesh(mesh.devices.reshape(2, 4, 8, 2, 2), ("yh", "x", "z", "yl", "core"))
    row, col = ("yh", "x"), ("z", "yl", "core")
    in_specs = (P(row, col), P(row, None), P(col, row), P(col, row), P(col, row))
    out_specs = (P(row, col), P(col, row), P(col, row))
    return jax.shard_map(per_device, mesh=own, in_specs=in_specs, out_specs=out_specs, check_vma=False)
```

```python
import jax
import jax.numpy as jnp
from jax import lax
from jax.sharding import Mesh, PartitionSpec as P


CHUNKS = (40, 32)
BASIS_CUTS = (384, 192)
beta_one = 0.9
beta_two = 0.95
epsilon = 1e-08
correct_one = 1.0 - 0.9**10
correct_two = 1.0 - 0.95**10
wide = jnp.float32
half = jnp.bfloat16
Y = ("yh", "yl")
OTHER_YL, OTHER_YH, OTHER_BOTH = 1, 2, 3


def shift(value, axis, by):
    size = lax.axis_size(axis)
    return lax.ppermute(value, axis, [(i, (i + by) % size) for i in range(size)])


def across(value, flip):
    return lax.ppermute(value, Y, [(i, i ^ flip) for i in range(4)])


def pick(blocks, index):
    return lax.dynamic_index_in_dim(blocks, index, 0, keepdims=False)


def add(*terms):
    total = terms[0].astype(wide)
    for term in terms[1:]:
        total = total + term.astype(wide)
    return total.astype(half)


def x_sum(own, right, far, left):
    far = shift(far, "x", 2)
    right = shift(right, "x", 1)
    left = shift(left, "x", -1)
    return add(own, right, left, far)


def x_gather(piece):
    far = shift(piece, "x", 2)
    return jnp.stack([piece, shift(piece, "x", -1), far, shift(piece, "x", 1)])


def z_sum(block):
    far = block(4)
    n = far.shape[1] // 2
    up = shift(far[:, :n], "z", 1)
    down = shift(far[:, n:], "z", -1)
    b = block(3)
    up = shift(jnp.concatenate([add(b[:, :n], up), b[:, n:]], axis=1), "z", 1)
    b = block(-3)
    down = shift(jnp.concatenate([b[:, :n], add(b[:, n:], down)], axis=1), "z", -1)
    for k in (2, 1):
        up = shift(add(block(k), up), "z", 1)
        down = shift(add(block(-k), down), "z", -1)
    return add(block(0), up, down)


def z_gather(piece):
    n = piece.shape[1] // 2
    got = {0: piece}
    up = down = piece
    for k in (1, 2, 3):
        up = got[8 - k] = shift(up, "z", 1)
        down = got[k] = shift(down, "z", -1)
    got[4] = jnp.concatenate([shift(up[:, :n], "z", 1), shift(down[:, n:], "z", -1)], axis=1)
    return jnp.stack([got[k] for k in range(8)])


def to_quarter(terms):
    from_yl = across(terms[1], OTHER_YL)
    from_both = across(terms[1], OTHER_BOTH)
    from_yh = across(terms[0], OTHER_YH)
    rows = jnp.concatenate([add(terms[0], from_yh), add(from_yl, from_both)], axis=-1)
    return jnp.concatenate([rows[0], shift(rows[1], "core", 1)], axis=-1)


def from_quarter(terms):
    n = terms.shape[-1] // 4
    rows = jnp.stack([terms[..., : 2 * n], shift(terms[..., 2 * n :], "core", 1)])
    own, other = rows[..., :n], rows[..., n:]
    from_yl = across(other, OTHER_YL)
    from_both = across(other, OTHER_BOTH)
    from_yh = across(own, OTHER_YH)
    return jnp.stack([add(own, from_yh), add(from_yl, from_both)])


def step_of(rotated, first_moment, second_moment):
    rotated = rotated.astype(wide)
    first_new = beta_one * first_moment + (1.0 - beta_one) * rotated
    second_new = beta_two * second_moment + (1.0 - beta_two) * rotated * rotated
    step = first_new / correct_one / (jnp.sqrt(second_new / correct_two) + epsilon)
    return step.astype(half), first_new, second_new


def seen_from_here(left_basis):
    x, yl, core = (lax.axis_index(a) for a in ("x", "yl", "core"))
    k = left_basis.shape[0]
    blocks = lax.optimization_barrier(left_basis.T).reshape(2, 4, 2, 2, -1, k)
    blocks = jnp.stack([lax.dynamic_index_in_dim(blocks, (x + i) % 4, 1, keepdims=False) for i in range(4)])
    blocks = jnp.stack([lax.dynamic_index_in_dim(blocks, (yl + i) % 2, 2, keepdims=False) for i in range(2)], 1)
    blocks = jnp.stack([lax.dynamic_index_in_dim(blocks, (core + i) % 2, 3, keepdims=False) for i in range(2)], 2)
    return blocks


def per_device(gradient, left_basis, right_basis, first_moment, second_moment):
    x, z = lax.axis_index("x"), lax.axis_index("z")
    n_cols = gradient.shape[1]
    rows = first_moment.shape[0]

    pieces, at = [], 0
    for size in BASIS_CUTS:
        pieces.append(across(right_basis[at : at + size], OTHER_YL))
        at += size
    own_half = [right_basis, *pieces]
    basis = jnp.concatenate(own_half + [shift(p, "core", 1) for p in own_half])

    left = lax.optimization_barrier(seen_from_here(left_basis))
    part = jnp.dot(left.reshape(-1, left.shape[-1]), gradient, preferred_element_type=wide).astype(half)
    part = part.reshape(4, 2, 2, 2, rows, n_cols)
    firsts, seconds, backs = [], [], []
    at = 0
    for h in CHUNKS:
        span = slice(at, at + h)
        at += h
        mine = x_sum(*(part[k, :, :, :, span] for k in range(4)))
        mine = to_quarter(mine)
        mine = x_gather(mine)
        right = jnp.dot(mine.reshape(8 * h, -1), basis, preferred_element_type=wide).astype(half)
        right = right.reshape(8, h, -1)
        rotated = z_sum(lambda k: pick(right, (z + k - x) % 4 * 2 + (z + k) // 4 % 2))
        step, first_new, second_new = step_of(rotated, first_moment[span], second_moment[span])
        firsts.append(first_new)
        seconds.append(second_new)
        steps = z_gather(step)
        back = lax.dot_general(
            steps.reshape(8 * h, -1), basis, (((1,), (1,)), ((), ())), preferred_element_type=wide
        ).astype(half)
        back = back.reshape(8, h, -1)
        block = lambda k: jnp.stack([pick(back, ((x + k) % 4 + i - z) % 8) for i in (0, 4)])
        back = x_sum(*(block(k) for k in range(4)))
        backs.append(x_gather(from_quarter(back)))
    back = jnp.concatenate(backs, axis=-2).reshape(-1, n_cols)
    update = lax.dot_general(
        left.reshape(-1, left.shape[-1]), back, (((0,), (0,)), ((), ())), preferred_element_type=wide
    ).astype(half)
    return update, jnp.concatenate(firsts), jnp.concatenate(seconds)


def solution(mesh):
    own = Mesh(mesh.devices.reshape(2, 4, 8, 2, 2), ("yh", "x", "z", "yl", "core"))
    row, col = ("yh", "x"), ("z", "yl", "core")
    in_specs = (P(row, col), P(row, None), P(col, row), P(col, row), P(col, row))
    out_specs = (P(row, col), P(col, row), P(col, row))

    return jax.shard_map(per_device, mesh=own, in_specs=in_specs, out_specs=out_specs, check_vma=False)
```

```python
import jax
import jax.numpy as jnp
from jax import lax
from jax.experimental import pallas as pl
from jax.experimental.pallas import tpu as pltpu
from jax.sharding import Mesh, PartitionSpec as P


CHUNKS = (40, 32)
BASIS_CUTS = (352, 224)
beta_one = 0.9
beta_two = 0.95
epsilon = 1e-08
correct_one = 1.0 - 0.9**10
correct_two = 1.0 - 0.95**10
wide = jnp.float32
half = jnp.bfloat16
Y = ("yh", "yl")
OTHER_YL, OTHER_YH, OTHER_BOTH = 1, 2, 3


def shift(value, axis, by):
    size = lax.axis_size(axis)
    return lax.ppermute(value, axis, [(i, (i + by) % size) for i in range(size)])


def across(value, flip):
    return lax.ppermute(value, Y, [(i, i ^ flip) for i in range(4)])


def pick(blocks, index):
    return lax.dynamic_index_in_dim(blocks, index, 0, keepdims=False)


def add(*terms):
    total = terms[0].astype(wide)
    for term in terms[1:]:
        total = total + term.astype(wide)
    return total.astype(half)


def x_sum(own, right, far, left):
    far = shift(far, "x", 2)
    right = shift(right, "x", 1)
    left = shift(left, "x", -1)
    return add(own, right, left, far)


def x_gather(piece):
    far = shift(piece, "x", 2)
    return jnp.stack([piece, shift(piece, "x", -1), far, shift(piece, "x", 1)])


def z_sum(block):
    far = block(4)
    n = far.shape[1] // 2
    up = shift(far[:, :n], "z", 1)
    down = shift(far[:, n:], "z", -1)
    b = block(3)
    up = shift(jnp.concatenate([add(b[:, :n], up), b[:, n:]], axis=1), "z", 1)
    b = block(-3)
    down = shift(jnp.concatenate([b[:, :n], add(b[:, n:], down)], axis=1), "z", -1)
    for k in (2, 1):
        up = shift(add(block(k), up), "z", 1)
        down = shift(add(block(-k), down), "z", -1)
    return add(block(0), up, down)


def z_gather(piece):
    n = piece.shape[1] // 2
    got = {0: piece}
    up = down = piece
    for k in (1, 2, 3):
        up = got[8 - k] = shift(up, "z", 1)
        down = got[k] = shift(down, "z", -1)
    got[4] = jnp.concatenate([shift(up[:, :n], "z", 1), shift(down[:, n:], "z", -1)], axis=1)
    return jnp.stack([got[k] for k in range(8)])


def first_kernel(left_ref, gradient_ref, *out_refs):
    gradient = gradient_ref[...]
    for k in range(4):
        part = jnp.dot(left_ref[k], gradient, preferred_element_type=wide).astype(half)
        part = part.reshape(2, 2, -1, part.shape[-1])
        at = 0
        for i in range(len(out_refs) // 4):
            out = out_refs[4 * i + k]
            h = out.shape[2]
            out[...] = part[:, :, at : at + h]
            at += h


def first_parts(left, gradient):
    left = left.reshape(4, -1, left.shape[-1])
    n = gradient.shape[1]
    shapes = [jax.ShapeDtypeStruct((2, 2, h, n), half) for h in CHUNKS for _ in range(4)]
    vmem = pl.BlockSpec(memory_space=pltpu.VMEM)
    flops = 2 * left.size * n
    outs = pl.pallas_call(
        first_kernel,
        out_shape=shapes,
        in_specs=[vmem, vmem],
        out_specs=[vmem] * len(shapes),
        cost_estimate=pl.CostEstimate(flops=flops, bytes_accessed=2 * 3 * left.size, transcendentals=0),
    )(left, gradient)
    return [outs[4 * i : 4 * i + 4] for i in range(len(CHUNKS))]


def y_sum(own, other):
    from_yl = across(other, OTHER_YL)
    from_both = across(other, OTHER_BOTH)
    from_yh = across(own, OTHER_YH)
    return add(own, from_yh), add(from_yl, from_both)


def from_quarter(terms):
    n = terms.shape[-1] // 4
    rows = jnp.stack(y_sum(terms[..., : 2 * n], terms[..., 2 * n :]))
    other = shift(rows[..., n:], "core", 1)
    return jnp.stack([rows[..., :n], other], axis=1)


def step_of(rotated, first_moment, second_moment):
    rotated = rotated.astype(wide)
    first_new = beta_one * first_moment + (1.0 - beta_one) * rotated
    second_new = beta_two * second_moment + (1.0 - beta_two) * rotated * rotated
    step = first_new / correct_one / (jnp.sqrt(second_new / correct_two) + epsilon)
    return step.astype(half), first_new, second_new


def seen_from_here(left_basis):
    x, yl, core = (lax.axis_index(a) for a in ("x", "yl", "core"))
    k = left_basis.shape[0]
    blocks = lax.optimization_barrier(left_basis.T).reshape(2, 4, 2, 2, -1, k)
    blocks = jnp.stack([lax.dynamic_index_in_dim(blocks, (x + i) % 4, 1, keepdims=False) for i in range(4)])
    blocks = jnp.stack([lax.dynamic_index_in_dim(blocks, (yl + i) % 2, 2, keepdims=False) for i in range(2)], 1)
    blocks = jnp.stack([lax.dynamic_index_in_dim(blocks, (core + i) % 2, 3, keepdims=False) for i in range(2)], 2)
    return blocks


def per_device(gradient, left_basis, right_basis, first_moment, second_moment):
    x, z = lax.axis_index("x"), lax.axis_index("z")
    n_cols = gradient.shape[1]

    pieces, at = [], 0
    for size in BASIS_CUTS:
        piece = right_basis if len(BASIS_CUTS) == 1 else right_basis[at : at + size]
        pieces.append(across(piece, OTHER_YL))
        at += size
    own_half = [right_basis, *pieces]
    swapped = [shift(p, "core", 1) for p in own_half]
    basis = jnp.concatenate([own_half[0], swapped[0], *own_half[1:], *swapped[1:]])
    gradient = jnp.concatenate([gradient, shift(gradient, "core", 1)], axis=1)
    left = lax.optimization_barrier(seen_from_here(left_basis))
    mines = []
    for part in first_parts(left[:, :, 0], gradient):
        mine = x_sum(*part)
        mine = jnp.concatenate(y_sum(mine[0], mine[1]), axis=-1)
        mines.append(x_gather(mine))
    firsts, seconds, backs = [], [], []
    at = 0
    for h, mine in zip(CHUNKS, mines):
        span = slice(at, at + h)
        at += h
        right = jnp.dot(mine.reshape(8 * h, -1), basis, preferred_element_type=wide).astype(half)
        right = right.reshape(8, h, -1)
        rotated = z_sum(lambda k: pick(right, (z + k - x) % 4 * 2 + (z + k) // 4 % 2))
        step, first_new, second_new = step_of(rotated, first_moment[span], second_moment[span])
        firsts.append(first_new)
        seconds.append(second_new)
        steps = z_gather(step)
        back = lax.dot_general(
            steps.reshape(8 * h, -1), basis, (((1,), (1,)), ((), ())), preferred_element_type=wide
        ).astype(half)
        back = back.reshape(8, h, -1)
        block = lambda k: jnp.stack([pick(back, ((x + k) % 4 + i - z) % 8) for i in (0, 4)])
        back = x_sum(*(block(k) for k in range(4)))
        back = from_quarter(back)
        backs.append(x_gather(back))
    back = jnp.concatenate(backs, axis=-2).reshape(-1, n_cols)
    update = lax.dot_general(
        left.reshape(-1, left.shape[-1]), back, (((0,), (0,)), ((), ())), preferred_element_type=wide
    ).astype(half)
    return update, jnp.concatenate(firsts), jnp.concatenate(seconds)


def solution(mesh):
    own = Mesh(mesh.devices.reshape(2, 4, 8, 2, 2), ("yh", "x", "z", "yl", "core"))
    row, col = ("yh", "x"), ("z", "yl", "core")
    in_specs = (P(row, col), P(row, None), P(col, row), P(col, row), P(col, row))
    out_specs = (P(row, col), P(col, row), P(col, row))

    return jax.shard_map(per_device, mesh=own, in_specs=in_specs, out_specs=out_specs, check_vma=False)
```

```python
import jax
import jax.numpy as jnp
from jax import lax
from jax.experimental import pallas as pl
from jax.experimental.pallas import tpu as pltpu
from jax.sharding import Mesh, PartitionSpec as P


CHUNKS = (32, 40)
BASIS_CUTS = (352, 224)
beta_one = 0.9
beta_two = 0.95
epsilon = 1e-08
correct_one = 1.0 - 0.9**10
correct_two = 1.0 - 0.95**10
wide = jnp.float32
half = jnp.bfloat16
Y = ("yh", "yl")
OTHER_YL, OTHER_YH, OTHER_BOTH = 1, 2, 3


def shift(value, axis, by):
    size = lax.axis_size(axis)
    return lax.ppermute(value, axis, [(i, (i + by) % size) for i in range(size)])


def across(value, flip):
    return lax.ppermute(value, Y, [(i, i ^ flip) for i in range(4)])


def pick(blocks, index):
    return lax.dynamic_index_in_dim(blocks, index, 0, keepdims=False)


def add(*terms):
    total = terms[0].astype(wide)
    for term in terms[1:]:
        total = total + term.astype(wide)
    return total.astype(half)


def x_sum(own, right, far, left):
    far = shift(far, "x", 2)
    right = shift(right, "x", 1)
    left = shift(left, "x", -1)
    return add(own, right, left, far)


def x_gather(piece):
    far = shift(piece, "x", 2)
    return jnp.stack([piece, shift(piece, "x", -1), far, shift(piece, "x", 1)])


def z_sum(block):
    far = block(4)
    n = far.shape[1] // 2
    up = shift(far[:, :n], "z", 1)
    down = shift(far[:, n:], "z", -1)
    b = block(3)
    up = shift(jnp.concatenate([add(b[:, :n], up), b[:, n:]], axis=1), "z", 1)
    b = block(-3)
    down = shift(jnp.concatenate([b[:, :n], add(b[:, n:], down)], axis=1), "z", -1)
    for k in (2, 1):
        up = shift(add(block(k), up), "z", 1)
        down = shift(add(block(-k), down), "z", -1)
    return add(block(0), up, down)


def z_gather(piece):
    n = piece.shape[1] // 2
    got = {0: piece}
    up = down = piece
    for k in (1, 2, 3):
        up = got[8 - k] = shift(up, "z", 1)
        down = got[k] = shift(down, "z", -1)
    got[4] = jnp.concatenate([shift(up[:, :n], "z", 1), shift(down[:, n:], "z", -1)], axis=1)
    return jnp.stack([got[k] for k in range(8)])


def first_kernel(left_ref, gradient_ref, *out_refs):
    gradient = gradient_ref[...]
    for k in range(4):
        part = jnp.dot(left_ref[k], gradient, preferred_element_type=wide).astype(half)
        part = part.reshape(2, 2, -1, part.shape[-1])
        at = 0
        for i in range(len(out_refs) // 4):
            out = out_refs[4 * i + k]
            h = out.shape[2]
            out[...] = part[:, :, at : at + h]
            at += h


def first_parts(left, gradient):
    left = left.reshape(4, -1, left.shape[-1])
    n = gradient.shape[1]
    shapes = [jax.ShapeDtypeStruct((2, 2, h, n), half) for h in CHUNKS for _ in range(4)]
    vmem = pl.BlockSpec(memory_space=pltpu.VMEM)
    flops = 2 * left.size * n
    outs = pl.pallas_call(
        first_kernel,
        out_shape=shapes,
        in_specs=[vmem, vmem],
        out_specs=[vmem] * len(shapes),
        cost_estimate=pl.CostEstimate(flops=flops, bytes_accessed=2 * 3 * left.size, transcendentals=0),
    )(left, gradient)
    return [outs[4 * i : 4 * i + 4] for i in range(len(CHUNKS))]


def y_sum(own, other):
    from_yl = across(other, OTHER_YL)
    from_both = across(other, OTHER_BOTH)
    from_yh = across(own, OTHER_YH)
    return add(own, from_yh), add(from_yl, from_both)


def from_quarter(terms):
    n = terms.shape[-1] // 4
    rows = jnp.stack(y_sum(terms[..., : 2 * n], terms[..., 2 * n :]))
    other = shift(rows[..., n:], "core", 1)
    return jnp.stack([rows[..., :n], other], axis=1)


def step_of(rotated, first_moment, second_moment):
    rotated = rotated.astype(wide)
    first_new = beta_one * first_moment + (1.0 - beta_one) * rotated
    second_new = beta_two * second_moment + (1.0 - beta_two) * rotated * rotated
    step = first_new / correct_one / (jnp.sqrt(second_new / correct_two) + epsilon)
    return step.astype(half), first_new, second_new


def seen_from_here(left_basis):
    x, yl, core = (lax.axis_index(a) for a in ("x", "yl", "core"))
    k = left_basis.shape[0]
    blocks = lax.optimization_barrier(left_basis.T).reshape(2, 4, 2, 2, -1, k)
    blocks = jnp.stack([lax.dynamic_index_in_dim(blocks, (x + i) % 4, 1, keepdims=False) for i in range(4)])
    blocks = jnp.stack([lax.dynamic_index_in_dim(blocks, (yl + i) % 2, 2, keepdims=False) for i in range(2)], 1)
    blocks = jnp.stack([lax.dynamic_index_in_dim(blocks, (core + i) % 2, 3, keepdims=False) for i in range(2)], 2)
    return blocks


def per_device(gradient, left_basis, right_basis, first_moment, second_moment):
    x, z = lax.axis_index("x"), lax.axis_index("z")
    n_cols = gradient.shape[1]

    pieces, at = [], 0
    for size in BASIS_CUTS:
        piece = right_basis if len(BASIS_CUTS) == 1 else right_basis[at : at + size]
        pieces.append(across(piece, OTHER_YL))
        at += size
    own_half = [right_basis, *pieces]
    count = right_basis.shape[0]
    basis = jnp.zeros((4 * count, right_basis.shape[1]), half)
    at = 0
    for piece in own_half:
        size = piece.shape[0]
        basis = lax.dynamic_update_slice(basis, piece, (at, 0))
        to = count if at == 0 else at + count
        basis = lax.dynamic_update_slice(basis, shift(piece, "core", 1), (to, 0))
        at += 2 * count if at == 0 else size
    gradient = jnp.concatenate([gradient, shift(gradient, "core", 1)], axis=1)
    left = lax.optimization_barrier(seen_from_here(left_basis))
    mines = []
    for part in first_parts(left[:, :, 0], gradient):
        mine = x_sum(*part)
        mine = jnp.concatenate(y_sum(mine[0], mine[1]), axis=-1)
        mines.append(x_gather(mine))
    firsts, seconds, backs = [], [], []
    at = 0
    for h, mine in zip(CHUNKS, mines):
        span = slice(at, at + h)
        at += h
        right = jnp.dot(mine.reshape(8 * h, -1), basis, preferred_element_type=wide).astype(half)
        right = right.reshape(8, h, -1)
        rotated = z_sum(lambda k: pick(right, (z + k - x) % 4 * 2 + (z + k) // 4 % 2))
        step, first_new, second_new = step_of(rotated, first_moment[span], second_moment[span])
        firsts.append(first_new)
        seconds.append(second_new)
        steps = z_gather(step)
        back = lax.dot_general(
            steps.reshape(8 * h, -1), basis, (((1,), (1,)), ((), ())), preferred_element_type=wide
        ).astype(half)
        back = back.reshape(8, h, -1)
        block = lambda k: jnp.stack([pick(back, ((x + k) % 4 + i - z) % 8) for i in (0, 4)])
        back = x_sum(*(block(k) for k in range(4)))
        back = from_quarter(back)
        backs.append(x_gather(back))
    back = jnp.concatenate(backs, axis=-2).reshape(-1, n_cols)
    update = lax.dot_general(
        left.reshape(-1, left.shape[-1]), back, (((0,), (0,)), ((), ())), preferred_element_type=wide
    ).astype(half)
    return update, jnp.concatenate(firsts), jnp.concatenate(seconds)


def solution(mesh):
    own = Mesh(mesh.devices.reshape(2, 4, 8, 2, 2), ("yh", "x", "z", "yl", "core"))
    row, col = ("yh", "x"), ("z", "yl", "core")
    in_specs = (P(row, col), P(row, None), P(col, row), P(col, row), P(col, row))
    out_specs = (P(row, col), P(col, row), P(col, row))

    return jax.shard_map(per_device, mesh=own, in_specs=in_specs, out_specs=out_specs, check_vma=False)
```
